32 devices in a mesh: epoch: 4 (over y, x), blend: 8 (over z, core).
Axes of the slice: x: 2, y: 2, z: 4, core: 2. Of those that a mesh axis runs over, the one named last changes fastest.
Arguments:
- visit_flux: bfloat16 [16, 32, 6, 16384], P('epoch', None, None, 'blend'), may hold values from -6 to 6
- visit_precision: bfloat16 [16, 32, 6, 16384], P('epoch', None, None, 'blend'), may hold values from 0.25 to 4
- visit_live: int32 [16, 32], P('epoch'), may hold values 0 or 1
- footprint: int32 [32, 8, 16384], P('blend', None, 'epoch'), may hold values 0 or 1
- source_count: int32 [32], P('blend'), may hold values from 1 to 8
- spectra_init: float32 [32, 8, 6], P('blend'), may hold values from 0.2 to 1.2
- morphology_init: float32 [32, 8, 16384], P('blend', None, 'epoch'), may hold values from 0 to 0.25
Outputs:
- coadd_flux: float32 [32, 6, 16384], P('blend', None, 'epoch')
- spectra: float32 [32, 8, 6], P('blend')
- morphology: float32 [32, 8, 16384], P('blend', None, 'epoch')
The draws below stay inside these ranges and needn't reach their ends.
All inputs are finite; a program needn't handle non-finite values. No bound on the sum of `visit_live` or of `footprint` on one device may be relied on, other than what follows from the above.
Results may differ from the reference program's by a relative error of at most 0.0003.
Values sent between devices are 32-bit elements; how exact they have to be, the bound alone decides.
A program may use at most 64 MiB of HBM per device.

```python
import math
import jax
import jax.numpy as jnp
from jax import lax

PIX = 16384
BANDS = 6
SRC = 8
ITERS = 2
EPOCHS = 16
BLENDS = 32


def with_ends(array, key, smallest, largest):
    dims = array.shape
    place = [jax.random.randint(jax.random.fold_in(key, axis), (), 0, dims[axis]) for axis in range(len(dims))]
    array = array.at[tuple(place)].set(smallest)
    longest = dims.index(max(dims))
    place[longest] = (place[longest] + 1) % dims[longest]
    return array.at[tuple(place)].set(largest)


def shard_levels(rng, shape, pieces, low, top_value):
    def one(position, blocks):
        draws = jax.random.uniform(jax.random.fold_in(jax.random.fold_in(rng, 6), position), (blocks,), jnp.float32, low / len(pieces), top_value / len(pieces))
        return jnp.repeat(jnp.exp(draws), shape[position] // blocks).reshape((-1,) + (1,) * (len(shape) - position - 1))

    gain = one(*pieces[0])
    for cut in pieces[1:]:
        gain = gain * one(*cut)
    return gain


def normal_values(own_key, extent, spread, bound, pieces=(), held_as=jnp.bfloat16):
    loudness = shard_levels(own_key, extent, pieces, -0.22, 0.18) if pieces else 1.0
    result = jax.random.normal(own_key, extent, jnp.float32) * spread * loudness
    return jnp.minimum(jnp.maximum(result, -bound), bound).astype(held_as)


def setup_inputs(seed: int = 0) -> dict:
    key_of = jax.random.split(jax.random.key(seed), 8)
    return {
        "visit_flux": normal_values(key_of[0], (EPOCHS, BLENDS, BANDS, PIX), 1.0, 6.0, ((0, 4), (3, 8))),
        "visit_precision": jnp.clip(jnp.exp(math.log(4.0) - 2.7725887 * jax.random.uniform(key_of[1], (EPOCHS, BLENDS, BANDS, PIX), jnp.float32) ** shard_levels(key_of[1], (EPOCHS, BLENDS, BANDS, PIX), ((0, 4), (3, 8)), -0.2, 0.2)), 0.25, 4.0).astype(jnp.bfloat16),
        "visit_live": with_ends((jax.random.randint(key_of[2], (EPOCHS, BLENDS), 0, 4) < 3).astype(jnp.int32), jax.random.fold_in(key_of[2], 1), 0, 1),
        "footprint": with_ends((jax.random.randint(key_of[3], (BLENDS, SRC, PIX), 0, 2) < 1).astype(jnp.int32), jax.random.fold_in(key_of[3], 1), 0, 1),
        "source_count": with_ends(jax.random.randint(key_of[4], (BLENDS,), 1, SRC + 1), jax.random.fold_in(key_of[4], 1), 1, SRC).astype(jnp.int32),
        "spectra_init": jnp.clip(0.2 + 1 * jax.random.uniform(key_of[5], (BLENDS, SRC, BANDS), jnp.float32) ** shard_levels(key_of[5], (BLENDS, SRC, BANDS), ((0, 8),), -0.2, 0.2), 0.2, 1.2),
        "morphology_init": jnp.clip(0.25 * jax.random.uniform(key_of[6], (BLENDS, SRC, PIX), jnp.float32) ** shard_levels(key_of[6], (BLENDS, SRC, PIX), ((0, 8), (2, 4)), -0.2, 0.2), 0.0, 0.25),
    }


def reference(visit_flux, visit_precision, visit_live, footprint, source_count, spectra_init, morphology_init):
    def accumulate(totals, visit):
        flux_one, precision_one, live_one = visit
        weights = precision_one.astype(jnp.float32) * live_one.astype(jnp.float32)[:, None, None]
        return (totals[0] + weights * flux_one.astype(jnp.float32), totals[1] + weights), None

    zeros = jnp.zeros(visit_flux.shape[1:], jnp.float32)
    (numerator, weight_sum), _ = lax.scan(accumulate, (zeros, zeros), (visit_flux, visit_precision, visit_live))
    coadd_flux = numerator / (1.0 + weight_sum)
    coverage = weight_sum / (1.0 + weight_sum)
    source_live = (jnp.arange(SRC, dtype=jnp.int32)[None, :] < source_count[:, None]).astype(jnp.float32)
    footprint_mask = footprint.astype(jnp.float32) * source_live[:, :, None]
    live_count = source_count.astype(jnp.float32)
    morphology = morphology_init * footprint_mask
    spectra = spectra_init
    highest = lax.Precision.HIGHEST
    for iteration in range(ITERS):
        blend_model = jnp.einsum("bkc,bkp->bcp", spectra, morphology, precision=highest)
        residual = coverage * (coadd_flux - blend_model)
        morph_grad = jnp.einsum("bkc,bcp->bkp", spectra, residual, precision=highest)
        morph_step = 1.0 / (1.0 + live_count[:, None] * jnp.sum(spectra * spectra, axis=2))
        morphology = jnp.maximum(0.0, morphology + morph_grad * morph_step[:, :, None]) * footprint_mask
        blend_model = jnp.einsum("bkc,bkp->bcp", spectra, morphology, precision=highest)
        residual = coverage * (coadd_flux - blend_model)
        spectra_grad = jnp.einsum("bkp,bcp->bkc", morphology, residual, precision=highest)
        morph_norm = jnp.sum(morphology * morphology, axis=2)
        spectra = jnp.maximum(0.0, spectra + spectra_grad / (1.0 + live_count[:, None] * morph_norm)[:, :, None])
    return coadd_flux, spectra, morphology
```

```python
import functools

import jax
import jax.numpy as jnp
from jax import lax
from jax.experimental import pallas as pl
from jax.experimental.pallas import tpu as pltpu
from jax.sharding import PartitionSpec as P

ITERS = 2


LANES = 128
MESH = pl.DeviceIdType.MESH


def factors(count):
    rows = max(d for d in range(1, count + 1) if count % d == 0 and d * d <= count)
    return rows, count // rows


def coadd_kernel(
    flux_hbm, prec_hbm, live_ref, foot_hbm, count_ref, spec_ref, morph_hbm,
    coadd_ref, spec_out, morph_ref,
    flux_v, prec_v, foot_v, cover,
    stage, land1, part, land2, final, pieces, by_band, by_source, step_ref, acc, sums,
    in_sem, side_sem, s1_send, s1_recv, s2_send, s2_recv, s3_send, s3_recv, ps_send, ps_recv,
    *, ne, nb, ny, nx,
):
    visits, every_blend, bands, block = flux_hbm.shape
    owned, slots, pix_part = morph_hbm.shape
    chunks = flux_v.shape[0]
    width = block // chunks
    per_dest = pix_part // block
    e = lax.axis_index("epoch")
    j = lax.axis_index("blend")
    y, x = e // nx, e % nx
    home_e = j // per_dest
    home_slot = j % per_dest
    f32 = jnp.float32

    def in_copy(q):
        window = pl.ds(q * width, width)
        return (
            pltpu.make_async_copy(flux_hbm.at[:, :, :, window], flux_v.at[q], in_sem.at[0, q]),
            pltpu.make_async_copy(prec_hbm.at[:, :, :, window], prec_v.at[q], in_sem.at[1, q]),
        )

    for q in range(chunks):
        for copy in in_copy(q):
            copy.start()
    side = (
        pltpu.make_async_copy(foot_hbm, foot_v, side_sem.at[0]),
        pltpu.make_async_copy(morph_hbm, morph_ref, side_sem.at[1]),
    )
    for copy in side:
        copy.start()

    barrier = pltpu.get_barrier_semaphore()
    total = ne * nb
    mine = e * nb + j

    def greet(d, carry):
        other = lax.rem(mine + d, total)
        pl.semaphore_signal(
            barrier, inc=1, device_id=(other // nb, lax.rem(other, nb)), device_id_type=MESH
        )
        return carry

    lax.fori_loop(1, total, greet, 0)

    def local_sum(q):
        for copy in in_copy(q):
            copy.wait()

        def one(dest, carry):
            for b in range(owned):
                blend = dest * owned + b
                num = None
                for v in range(visits):
                    w = prec_v[q, v, blend].astype(f32) * live_ref[v, blend].astype(f32)
                    n = w * flux_v[q, v, blend].astype(f32)
                    num, wsum = (n, w) if num is None else (num + n, wsum + w)
                for p in range(ne):
                    py, px = p // nx, p % nx
                    lanes = slice(p * LANES, (p + 1) * LANES)
                    rows = slice(b * bands, (b + 1) * bands)
                    stage[0, q, px * ny + py, dest, rows, :] = num[:, lanes]
                    stage[1, q, py * nx + px, dest, rows, :] = wsum[:, lanes]
            return carry

        lax.fori_loop(0, nb, one, 0)

    def line(a, first):
        along_x = (a == 0) == first
        return (x, nx) if along_x else (y, ny)

    def device_at(a, first, where):
        along_x = (a == 0) == first
        return (y * nx + where if along_x else where * nx + x, j)

    def s1(a, q, d):
        at, n = line(a, True)
        other = line(a, False)[1]
        to = lax.rem(at + d, n)
        return pltpu.make_async_remote_copy(
            src_ref=stage.at[a, q, pl.ds(to * other, other)],
            dst_ref=land1.at[a, q, d - 1],
            send_sem=s1_send.at[a, q, d - 1], recv_sem=s1_recv.at[a, q, d - 1],
            device_id=device_at(a, True, to), device_id_type=MESH,
        )

    def s2(a, q, d):
        at, n = line(a, False)
        to = lax.rem(at + d, n)
        return pltpu.make_async_remote_copy(
            src_ref=part.at[a, q, to],
            dst_ref=land2.at[a, q, d - 1],
            send_sem=s2_send.at[a, q, d - 1], recv_sem=s2_recv.at[a, q, d - 1],
            device_id=device_at(a, False, to), device_id_type=MESH,
        )

    def s1_start(q):
        for a in range(2):
            for d in range(1, line(a, True)[1]):
                s1(a, q, d).start()

    def s2_start(q):
        for a in range(2):
            at, n = line(a, True)
            others = line(a, False)[1]
            for d in range(1, n):
                s1(a, q, d).wait_recv()

            def add(i, carry):
                o, dest = i // nb, lax.rem(i, nb)
                v = stage[a, q, at * others + o, dest]
                for d in range(1, n):
                    v = v + land1[a, q, d - 1, o, dest]
                part[a, q, o, dest] = v
                return carry

            lax.fori_loop(0, others * nb, add, 0)
            for d in range(1, others):
                s2(a, q, d).start()

    here = home_e == e

    def s3_local(q):
        return pltpu.make_async_copy(
            final.at[q, j],
            pieces.at[q, :, :, pl.ds(pl.multiple_of(home_slot * width + e * LANES, LANES), LANES)],
            s3_recv.at[q],
        )

    def s3_remote(q, to):
        return pltpu.make_async_remote_copy(
            src_ref=final.at[q, to],
            dst_ref=pieces.at[
                q, :, :, pl.ds(pl.multiple_of(home_slot * width + e * LANES, LANES), LANES)
            ],
            send_sem=s3_send.at[q, to], recv_sem=s3_recv.at[q],
            device_id=(home_e, to), device_id_type=MESH,
        )

    def s3_start(q):
        for a in range(2):
            at, n = line(a, False)
            for d in range(1, n):
                s2(a, q, d).wait_recv()

            def add(dest, carry):
                v = part[a, q, at, dest]
                for d in range(1, n):
                    v = v + land2[a, q, d - 1, dest]
                final[q, dest, a] = v
                return carry

            lax.fori_loop(0, nb, add, 0)

        def send(d, carry):
            to = lax.rem(j + d, nb)
            s3_remote(q, to).start()
            return carry

        lax.fori_loop(1, nb, send, 0)

        @pl.when(here)
        def _():
            s3_local(q).start()

        @pl.when(jnp.logical_not(here))
        def _():
            s3_remote(q, j).start()

    sub = lax.broadcasted_iota(jnp.int32, (slots, LANES), 0)
    lane = lax.broadcasted_iota(jnp.int32, (slots, LANES), 1)

    def spread():
        for b in range(owned):
            norm = None
            for c in range(bands):
                s = by_band[b, c]
                norm = s * s if norm is None else norm + s * s
            step_ref[b] = 1.0 / (1.0 + count_ref[b].astype(f32) * norm)

        def move(b, carry):
            for k in range(slots):
                for c in range(bands):
                    by_source[b, k, c : c + 1, :] = by_band[b, c, k : k + 1, :]
            return carry

        lax.fori_loop(0, owned, move, 0)

    def deblend(b, start, first):
        live = jnp.where(sub < count_ref[b], 1.0, 0.0).astype(f32)
        step = step_ref[b]
        bs = [by_source[b, k] for k in range(slots)]
        bb = [by_band[b, c] for c in range(bands)]
        grads = [acc[b, c] for c in range(bands + 1)]

        for t in range(width // LANES):
            px = pl.ds(pl.multiple_of(start + t * LANES, LANES), LANES)
            mask = foot_v[b, :, px].astype(f32) * live
            morph = morph_ref[b, :, px]
            if first:
                morph = morph * mask
            cov = cover[b, :, px]
            flux = coadd_ref[b, :, px]

            def residual(m):
                model = bs[0] * m[0:1, :]
                for k in range(1, slots):
                    model = model + bs[k] * m[k : k + 1, :]
                return cov * (flux - model)

            res = residual(morph)
            grad = bb[0] * res[0:1, :]
            for c in range(1, bands):
                grad = grad + bb[c] * res[c : c + 1, :]
            morph = jnp.maximum(0.0, morph + grad * step) * mask
            morph_ref[b, :, px] = morph
            res = residual(morph)
            for c in range(bands):
                grads[c] = grads[c] + morph * res[c : c + 1, :]
            grads[bands] = grads[bands] + morph * morph
        for c in range(bands + 1):
            acc[b, c] = grads[c]

    def finish(q):
        pltpu.make_async_copy(pieces.at[q], pieces.at[q], s3_recv.at[q]).wait()
        for s in range(per_dest):
            src = slice(s * width, (s + 1) * width)
            dst = slice(s * block + q * width, s * block + (q + 1) * width)
            for b in range(owned):
                rows = slice(b * bands, (b + 1) * bands)
                wsum = pieces[q, 1, rows, src]
                inv = 1.0 / (1.0 + wsum)
                coadd_ref[b, :, dst] = pieces[q, 0, rows, src] * inv
                cover[b, :, dst] = wsum * inv

        def go(i, carry):
            s, b = i // owned, lax.rem(i, owned)
            deblend(b, s * block + q * width, True)
            return carry

        lax.fori_loop(0, per_dest * owned, go, 0)

    def ps_copy(it, d):
        to = lax.rem(e + d, ne)
        return pltpu.make_async_remote_copy(
            src_ref=sums.at[it, 0], dst_ref=sums.at[it, d],
            send_sem=ps_send.at[it, d - 1], recv_sem=ps_recv.at[it, d - 1],
            device_id=(to, j), device_id_type=MESH,
        )

    def update(it):
        packed = jnp.zeros((slots, LANES), f32)
        for b in range(owned):
            for c in range(bands + 1):
                total_bc = jnp.sum(acc[b, c], axis=1, keepdims=True)
                packed = jnp.where(lane == b * (bands + 1) + c, total_bc, packed)
        sums[it, 0] = packed
        for d in range(1, ne):
            ps_copy(it, d).start()
        for d in range(1, ne):
            ps_copy(it, d).wait_recv()
        whole = None
        for o in range(ne):
            slot = lax.rem(e - o + ne, ne)
            v = sums[it, slot]
            whole = v if whole is None else whole + v
        for b in range(owned):
            at = b * (bands + 1)
            norm = whole[:, at + bands : at + bands + 1]
            scale = 1.0 / (1.0 + count_ref[b].astype(f32) * norm)
            for c in range(bands):
                grad = jnp.broadcast_to(whole[:, at + c : at + c + 1] * scale, (slots, LANES))
                by_band[b, c] = jnp.maximum(0.0, by_band[b, c] + grad)

    acc[...] = jnp.zeros_like(acc)
    for b in range(owned):
        for c in range(bands):
            by_band[b, c] = jnp.broadcast_to(spec_ref[b, :, c : c + 1], (slots, LANES))
    spread()

    local_sum(0)
    pl.semaphore_wait(barrier, total - 1)
    s1_start(0)
    if chunks > 1:
        local_sum(1)
        s1_start(1)
    for copy in side:
        copy.wait()
    for q in range(chunks + 2):
        if q < chunks:
            s2_start(q)
        if q + 2 < chunks:
            local_sum(q + 2)
            s1_start(q + 2)
        if 0 <= q - 1 < chunks:
            s3_start(q - 1)
        if 0 <= q - 2 < chunks:
            finish(q - 2)

    update(0)
    spread()
    for it in range(1, ITERS):
        acc[...] = jnp.zeros_like(acc)

        def again(i, carry):
            w, b = i // owned, lax.rem(i, owned)
            deblend(b, w * width, False)
            return carry

        lax.fori_loop(0, owned * (pix_part // width), again, 0)
        update(it)
        if it + 1 < ITERS:
            spread()
    for b in range(owned):
        out = by_band[b, 0]
        for c in range(1, bands):
            out = jnp.where(lane == c, by_band[b, c], out)
        spec_out[b] = out[:, :bands]

    for q in range(chunks):
        for a in range(2):
            for d in range(1, line(a, True)[1]):
                s1(a, q, d).wait_send()
            for d in range(1, line(a, False)[1]):
                s2(a, q, d).wait_send()

        def sent(d, carry, q=q):
            s3_remote(q, lax.rem(j + d, nb)).wait_send()
            return carry

        lax.fori_loop(1, nb, sent, 0)

        @pl.when(jnp.logical_not(here))
        def _(q=q):
            s3_remote(q, j).wait_send()

    for it in range(ITERS):
        for d in range(1, ne):
            ps_copy(it, d).wait_send()


def fused(ne, nb, visit_flux, visit_precision, visit_live, footprint, source_count, spectra_init,
          morphology_init):
    visits, every_blend, bands, block = visit_flux.shape
    owned, slots, pix_part = morphology_init.shape
    ny, nx = factors(ne)
    width = ne * LANES
    chunks = block // width
    per_dest = pix_part // block
    rows = owned * bands
    hop = max(nx, ny) - 1
    f32 = jnp.float32
    vmem, smem, hbm = (pl.BlockSpec(memory_space=s) for s in (pltpu.VMEM, pltpu.SMEM, pl.ANY))
    dma = pltpu.SemaphoreType.DMA
    return pl.pallas_call(
        functools.partial(coadd_kernel, ne=ne, nb=nb, ny=ny, nx=nx),
        out_shape=(
            jax.ShapeDtypeStruct((owned, bands, pix_part), f32),
            jax.ShapeDtypeStruct((owned, slots, bands), f32),
            jax.ShapeDtypeStruct((owned, slots, pix_part), f32),
        ),
        in_specs=[hbm, hbm, smem, hbm, smem, vmem, hbm],
        out_specs=(vmem, vmem, vmem),
        scratch_shapes=[
            pltpu.VMEM((chunks, visits, every_blend, bands, width), visit_flux.dtype),
            pltpu.VMEM((chunks, visits, every_blend, bands, width), visit_precision.dtype),
            pltpu.VMEM((owned, slots, pix_part), jnp.int32),
            pltpu.VMEM((owned, bands, pix_part), f32),
            pltpu.VMEM((2, chunks, ne, nb, rows, LANES), f32),
            pltpu.VMEM((2, chunks, hop, max(nx, ny), nb, rows, LANES), f32),
            pltpu.VMEM((2, chunks, max(nx, ny), nb, rows, LANES), f32),
            pltpu.VMEM((2, chunks, hop, nb, rows, LANES), f32),
            pltpu.VMEM((chunks, nb, 2, rows, LANES), f32),
            pltpu.VMEM((chunks, 2, rows, per_dest * width), f32),
            pltpu.VMEM((owned, bands, slots, LANES), f32),
            pltpu.VMEM((owned, slots, bands, LANES), f32),
            pltpu.VMEM((owned, slots, LANES), f32),
            pltpu.VMEM((owned, bands + 1, slots, LANES), f32),
            pltpu.VMEM((ITERS, ne, slots, LANES), f32),
            dma((2, chunks)),
            dma((2,)),
            dma((2, chunks, hop)),
            dma((2, chunks, hop)),
            dma((2, chunks, hop)),
            dma((2, chunks, hop)),
            dma((chunks, nb)),
            dma((chunks,)),
            dma((ITERS, ne - 1)),
            dma((ITERS, ne - 1)),
        ],
        compiler_params=pltpu.CompilerParams(
            collective_id=0, has_side_effects=True, vmem_limit_bytes=56 * 2**20
        ),
    )(visit_flux, visit_precision, visit_live, footprint, source_count, spectra_init,
      morphology_init)


def on_device(
    visit_flux, visit_precision, visit_live, footprint, source_count, spectra_init, morphology_init
):
    weights = visit_precision.astype(jnp.float32) * visit_live.astype(jnp.float32)[:, :, None, None]
    numerator = jnp.sum(weights * visit_flux.astype(jnp.float32), axis=0)
    weight_sum = jnp.sum(weights, axis=0)
    pix_part = morphology_init.shape[2]
    owned = morphology_init.shape[0]
    numerator, weight_sum = (
        lax.psum_scatter(numerator, "epoch", scatter_dimension=2, tiled=True),
        lax.psum_scatter(weight_sum, "epoch", scatter_dimension=2, tiled=True),
    )
    every_blend, band_count, piece = numerator.shape
    numerator = numerator.reshape(every_blend, band_count, 1, piece)
    weight_sum = weight_sum.reshape(every_blend, band_count, 1, piece)
    numerator, weight_sum = (
        lax.all_to_all(numerator, "blend", split_axis=0, concat_axis=2, tiled=True),
        lax.all_to_all(weight_sum, "blend", split_axis=0, concat_axis=2, tiled=True),
    )
    blocks = numerator.shape[2]
    numerator = numerator.reshape(owned, band_count, blocks, 1, piece)
    weight_sum = weight_sum.reshape(owned, band_count, blocks, 1, piece)
    numerator, weight_sum = (
        lax.all_to_all(numerator, "epoch", split_axis=2, concat_axis=3, tiled=True),
        lax.all_to_all(weight_sum, "epoch", split_axis=2, concat_axis=3, tiled=True),
    )
    numerator = numerator.reshape(owned, band_count, pix_part)
    weight_sum = weight_sum.reshape(owned, band_count, pix_part)
    coadd_flux = numerator / (1.0 + weight_sum)
    coverage = weight_sum / (1.0 + weight_sum)
    slots = footprint.shape[1]
    source_live = (jnp.arange(slots, dtype=jnp.int32)[None, :] < source_count[:, None]).astype(
        jnp.float32
    )
    footprint_mask = footprint.astype(jnp.float32) * source_live[:, :, None]
    live_count = source_count.astype(jnp.float32)
    morphology = morphology_init * footprint_mask
    spectra = spectra_init
    highest = lax.Precision.HIGHEST
    for iteration in range(ITERS):
        blend_model = jnp.einsum("bkc,bkp->bcp", spectra, morphology, precision=highest)
        residual = coverage * (coadd_flux - blend_model)
        morph_grad = jnp.einsum("bkc,bcp->bkp", spectra, residual, precision=highest)
        morph_step = 1.0 / (1.0 + live_count[:, None] * jnp.sum(spectra * spectra, axis=2))
        morphology = (
            jnp.maximum(0.0, morphology + morph_grad * morph_step[:, :, None]) * footprint_mask
        )
        blend_model = jnp.einsum("bkc,bkp->bcp", spectra, morphology, precision=highest)
        residual = coverage * (coadd_flux - blend_model)
        spectra_grad = jnp.einsum("bkp,bcp->bkc", morphology, residual, precision=highest)
        morph_norm = jnp.sum(morphology * morphology, axis=2)
        spectra_grad, morph_norm = lax.psum((spectra_grad, morph_norm), "epoch")
        spectra = jnp.maximum(
            0.0, spectra + spectra_grad / (1.0 + live_count[:, None] * morph_norm)[:, :, None]
        )
    return (coadd_flux, spectra, morphology)


def solution(mesh):
    ne, nb = mesh.shape["epoch"], mesh.shape["blend"]

    def step(visit_flux, visit_precision, visit_live, footprint, source_count, spectra_init,
             morphology_init):
        block, bands = visit_flux.shape[3], visit_flux.shape[2]
        owned, pix_part = morphology_init.shape[0], morphology_init.shape[2]
        ny, nx = factors(ne)
        fits = (
            block % (ne * LANES) == 0
            and pix_part % block == 0
            and min(ny, nx) > 1
            and owned * (bands + 1) <= LANES
        )
        run = functools.partial(fused, ne, nb) if fits else on_device
        return run(visit_flux, visit_precision, visit_live, footprint, source_count, spectra_init,
                   morphology_init)

    in_specs = (
        P("epoch", None, None, "blend"),
        P("epoch", None, None, "blend"),
        P("epoch", None),
        P("blend", None, "epoch"),
        P("blend"),
        P("blend", None, None),
        P("blend", None, "epoch"),
    )
    out_specs = (P("blend", None, "epoch"), P("blend", None, None), P("blend", None, "epoch"))
    return jax.shard_map(
        step, mesh=mesh, in_specs=in_specs, out_specs=out_specs, check_vma=False
    )
```

```python
import functools

import jax
import jax.numpy as jnp
from jax import lax
from jax.experimental import pallas as pl
from jax.experimental.pallas import tpu as pltpu
from jax.sharding import PartitionSpec as P

ITERS = 2


LANES = 128
MESH = pl.DeviceIdType.MESH


def factors(count):
    rows = max(d for d in range(1, count + 1) if count % d == 0 and d * d <= count)
    return rows, count // rows


def coadd_kernel(
    flux_hbm, prec_hbm, live_ref, foot_hbm, count_ref, spec_ref, morph_hbm,
    coadd_ref, spec_out, morph_ref,
    flux_v, prec_v, foot_v, flux_c, cover,
    stage, land1, part, land2, final, pieces, spectra, step_ref, acc, sums,
    in_sem, side_sem, s1_send, s1_recv, s2_send, s2_recv, s3_send, s3_recv, ps_send, ps_recv,
    *, ne, nb, ny, nx,
):
    visits, bands, every_blend, block = flux_hbm.shape
    owned, slots, pix_part = morph_hbm.shape
    chunks = flux_v.shape[0]
    width = block // chunks
    per_dest = pix_part // block
    held = per_dest * owned
    e = lax.axis_index("epoch")
    j = lax.axis_index("blend")
    y, x = e // nx, e % nx
    home_e = j // per_dest
    home_slot = j % per_dest
    f32 = jnp.float32

    def in_copy(q):
        window = pl.ds(q * width, width)
        return (
            pltpu.make_async_copy(prec_hbm.at[:, :, :, window], prec_v.at[q], in_sem.at[0, q]),
            pltpu.make_async_copy(flux_hbm.at[:, :, :, window], flux_v.at[q], in_sem.at[1, q]),
        )

    side = []
    for s in range(per_dest):
        for b in range(owned):
            row = s * owned + b
            window = pl.ds(s * block, block)
            side.append(pltpu.make_async_copy(
                foot_hbm.at[b, :, window], foot_v.at[:, row, :], side_sem.at[0, row]))
            side.append(pltpu.make_async_copy(
                morph_hbm.at[b, :, window], morph_ref.at[:, row, :], side_sem.at[1, row]))

    for q in range(chunks):
        for copy in in_copy(q):
            copy.start()

    barrier = pltpu.get_barrier_semaphore()
    total = ne * nb
    mine = e * nb + j

    def greet(d, carry):
        other = lax.rem(mine + d, total)
        pl.semaphore_signal(
            barrier, inc=1, device_id=(other // nb, lax.rem(other, nb)), device_id_type=MESH
        )
        return carry

    lax.fori_loop(1, total, greet, 0)

    square_r = lax.broadcasted_iota(jnp.int32, (every_blend, every_blend), 0)
    square_c = lax.broadcasted_iota(jnp.int32, (every_blend, every_blend), 1)
    lives = []
    for v in range(visits):
        row = jnp.broadcast_to(live_ref[v : v + 1, :].astype(f32), (every_blend, every_blend))
        column = jnp.sum(jnp.where(square_r == square_c, row, 0.0), axis=1, keepdims=True)
        lives.append(jnp.broadcast_to(column, (every_blend, LANES)))

    def local_sum(q):
        for copy in in_copy(q):
            copy.wait()

        def one(c, carry):
            for p in range(ne):
                lanes = slice(p * LANES, (p + 1) * LANES)
                py, px = p // nx, p % nx
                num = None
                for v in range(visits):
                    w = prec_v[q, v, c, :, lanes].astype(f32) * lives[v]
                    n = w * flux_v[q, v, c, :, lanes].astype(f32)
                    num, wsum = (n, w) if num is None else (num + n, wsum + w)
                stage[0, q, px * ny + py, c] = num
                stage[1, q, py * nx + px, c] = wsum
            return carry

        lax.fori_loop(0, bands, one, 0)

    def line(a, first):
        along_x = (a == 0) == first
        return (x, nx) if along_x else (y, ny)

    def device_at(a, first, where):
        along_x = (a == 0) == first
        return (y * nx + where if along_x else where * nx + x, j)

    def s1(a, q, d):
        at, n = line(a, True)
        other = line(a, False)[1]
        to = lax.rem(at + d, n)
        return pltpu.make_async_remote_copy(
            src_ref=stage.at[a, q, pl.ds(to * other, other)],
            dst_ref=land1.at[a, q, d - 1],
            send_sem=s1_send.at[a, q, d - 1], recv_sem=s1_recv.at[a, q, d - 1],
            device_id=device_at(a, True, to), device_id_type=MESH,
        )

    def s2(a, q, d):
        at, n = line(a, False)
        to = lax.rem(at + d, n)
        return pltpu.make_async_remote_copy(
            src_ref=part.at[a, q, to],
            dst_ref=land2.at[a, q, d - 1],
            send_sem=s2_send.at[a, q, d - 1], recv_sem=s2_recv.at[a, q, d - 1],
            device_id=device_at(a, False, to), device_id_type=MESH,
        )

    def s1_start(q):
        for a in range(2):
            for d in range(1, line(a, True)[1]):
                s1(a, q, d).start()

    def s2_start(q):
        for a in range(2):
            at, n = line(a, True)
            others = line(a, False)[1]
            for d in range(1, n):
                s1(a, q, d).wait_recv()

            def add(c, carry):
                for o in range(others):
                    v = stage[a, q, at * others + o, c]
                    for d in range(1, n):
                        v = v + land1[a, q, d - 1, o, c]
                    part[a, q, o, c] = v
                return carry

            lax.fori_loop(0, bands, add, 0)
            for d in range(1, others):
                s2(a, q, d).start()

    here = home_e == e

    def landing(q):
        lanes = pl.ds(pl.multiple_of(e * LANES, LANES), LANES)
        return pieces.at[q, :, :, home_slot, :, lanes]

    def s3_local(q):
        return pltpu.make_async_copy(final.at[q, j], landing(q), s3_recv.at[q])

    def s3_remote(q, to):
        return pltpu.make_async_remote_copy(
            src_ref=final.at[q, to], dst_ref=landing(q),
            send_sem=s3_send.at[q, to], recv_sem=s3_recv.at[q],
            device_id=(home_e, to), device_id_type=MESH,
        )

    def s3_start(q):
        for a in range(2):
            at, n = line(a, False)
            for d in range(1, n):
                s2(a, q, d).wait_recv()

            def add(c, carry):
                v = part[a, q, at, c]
                for d in range(1, n):
                    v = v + land2[a, q, d - 1, c]
                for to in range(nb):
                    final[q, to, a, c] = v[to * owned : (to + 1) * owned, :]
                return carry

            lax.fori_loop(0, bands, add, 0)

        def send(d, carry):
            s3_remote(q, lax.rem(j + d, nb)).start()
            return carry

        lax.fori_loop(1, nb, send, 0)

        @pl.when(here)
        def _():
            s3_local(q).start()

        @pl.when(jnp.logical_not(here))
        def _():
            s3_remote(q, j).start()

    sub = lax.broadcasted_iota(jnp.int32, (held, LANES), 0)
    lane = lax.broadcasted_iota(jnp.int32, (held, LANES), 1)
    count = jnp.zeros((held, LANES), jnp.int32)
    for b in range(owned):
        count = jnp.where(lax.rem(sub, owned) == b, count_ref[b], count)
    live_count = count.astype(f32)

    def steps():
        for k in range(slots):
            norm = None
            for c in range(bands):
                s = spectra[k, c]
                norm = s * s if norm is None else norm + s * s
            step_ref[k] = 1.0 / (1.0 + live_count * norm)

    group = 2

    def deblend(start, first):
        runs = [
            pl.ds(pl.multiple_of(start + t * LANES, LANES), LANES) for t in range(group)
        ]

        def masks(k):
            live = jnp.where(count > k, 1.0, 0.0).astype(f32)
            return [foot_v[k, :, px].astype(f32) * live for px in runs]

        def residual(morph):
            res = []
            for c in range(bands):
                model = [None] * group
                for k in range(slots):
                    s = spectra[k, c]
                    for t in range(group):
                        v = s * morph[k][t]
                        model[t] = v if k == 0 else model[t] + v
                res.append([
                    cover[c, :, px] * (flux_c[c, :, px] - model[t]) for t, px in enumerate(runs)
                ])
            return res

        morph = []
        for k in range(slots):
            m = [morph_ref[k, :, px] for px in runs]
            morph.append([a * b for a, b in zip(m, masks(k))] if first else m)
        res = residual(morph)
        for k in range(slots):
            mask = masks(k)
            grad = [None] * group
            for c in range(bands):
                s = spectra[k, c]
                for t in range(group):
                    v = s * res[c][t]
                    grad[t] = v if c == 0 else grad[t] + v
            step = step_ref[k]
            for t, px in enumerate(runs):
                m = jnp.maximum(0.0, morph[k][t] + grad[t] * step) * mask[t]
                morph[k][t] = m
                morph_ref[k, :, px] = m
        res = residual(morph)
        for k in range(slots):
            for c in range(bands):
                v = acc[k, c]
                for t in range(group):
                    v = v + morph[k][t] * res[c][t]
                acc[k, c] = v
            v = acc[k, bands]
            for t in range(group):
                v = v + morph[k][t] * morph[k][t]
            acc[k, bands] = v

    def finish(q):
        pltpu.make_async_copy(pieces.at[q], pieces.at[q], s3_recv.at[q]).wait()
        at = slice(q * width, (q + 1) * width)

        def unpack(c, carry):
            for s in range(per_dest):
                rows = slice(s * owned, (s + 1) * owned)
                wsum = pieces[q, 1, c, s]
                inv = 1.0 / (1.0 + wsum)
                flux = pieces[q, 0, c, s] * inv
                coadd_ref[c, :, s * block + q * width : s * block + (q + 1) * width] = flux
                flux_c[c, rows, at] = flux
                cover[c, rows, at] = wsum * inv
            return carry

        lax.fori_loop(0, bands, unpack, 0)

        def go(i, carry):
            deblend(q * width + i * (group * LANES), True)
            return carry

        lax.fori_loop(0, width // (group * LANES), go, 0)

    def ps_copy(it, d):
        to = lax.rem(e + d, ne)
        return pltpu.make_async_remote_copy(
            src_ref=sums.at[it, 0], dst_ref=sums.at[it, d],
            send_sem=ps_send.at[it, d - 1], recv_sem=ps_recv.at[it, d - 1],
            device_id=(to, j), device_id_type=MESH,
        )

    def update(it):
        packed = jnp.zeros((held, LANES), f32)
        for k in range(slots):
            for c in range(bands + 1):
                whole = jnp.sum(acc[k, c], axis=1, keepdims=True)
                packed = jnp.where(lane == k * (bands + 1) + c, whole, packed)
        sums[it, 0] = packed
        for d in range(1, ne):
            ps_copy(it, d).start()
        for d in range(1, ne):
            ps_copy(it, d).wait_recv()
        whole = None
        for o in range(ne):
            v = sums[it, lax.rem(e - o + ne, ne)]
            whole = v if whole is None else whole + v
        one = whole[0:owned, :]
        for s in range(1, per_dest):
            one = one + whole[s * owned : (s + 1) * owned, :]
        whole = jnp.concatenate([one] * per_dest, axis=0)
        for k in range(slots):
            at = k * (bands + 1)
            norm = jnp.broadcast_to(whole[:, at + bands : at + bands + 1], (held, LANES))
            scale = 1.0 / (1.0 + live_count * norm)
            for c in range(bands):
                grad = jnp.broadcast_to(whole[:, at + c : at + c + 1], (held, LANES))
                spectra[k, c] = jnp.maximum(0.0, spectra[k, c] + grad * scale)

    local_sum(0)
    pl.semaphore_wait(barrier, total - 1)
    s1_start(0)
    if chunks > 1:
        local_sum(1)
        s1_start(1)
    for copy in side:
        copy.start()

    acc[...] = jnp.zeros_like(acc)
    for k in range(slots):
        for c in range(bands):
            start = jnp.broadcast_to(spec_ref[c, :, k : k + 1], (owned, LANES))
            spectra[k, c] = jnp.concatenate([start] * per_dest, axis=0)
    steps()

    for q in range(chunks + 2):
        if q < chunks:
            s2_start(q)
        if q + 2 < chunks:
            local_sum(q + 2)
            s1_start(q + 2)
        if 0 <= q - 1 < chunks:
            s3_start(q - 1)
        if q == 2:
            for copy in side:
                copy.wait()
        if 0 <= q - 2 < chunks:
            finish(q - 2)

    update(0)
    for it in range(1, ITERS):
        steps()
        acc[...] = jnp.zeros_like(acc)

        def again(i, carry):
            deblend(i * (group * LANES), False)
            return carry

        lax.fori_loop(0, block // (group * LANES), again, 0)
        update(it)
    for c in range(bands):
        out = spectra[0, c]
        for k in range(1, slots):
            out = jnp.where(lane == k, spectra[k, c], out)
        spec_out[c] = out[0:owned, :slots]

    for q in range(chunks):
        for a in range(2):
            for d in range(1, line(a, True)[1]):
                s1(a, q, d).wait_send()
            for d in range(1, line(a, False)[1]):
                s2(a, q, d).wait_send()

        def sent(d, carry, q=q):
            s3_remote(q, lax.rem(j + d, nb)).wait_send()
            return carry

        lax.fori_loop(1, nb, sent, 0)

        @pl.when(jnp.logical_not(here))
        def _(q=q):
            s3_remote(q, j).wait_send()

    for it in range(ITERS):
        for d in range(1, ne):
            ps_copy(it, d).wait_send()


def hand_over(coadd_in, spec_in, morph_in, coadd_out, spec_out, morph_out, sems, row_sems):
    owned, _, pix_part = morph_out.shape
    _, held, block = morph_in.shape
    copies = [
        pltpu.make_async_copy(morph_in.at[:, row, :],
                              morph_out.at[row % owned, :, pl.ds(row // owned * block, block)],
                              row_sems.at[row])
        for row in range(held)
    ]
    copies.append(pltpu.make_async_copy(coadd_in, coadd_out, sems.at[0]))
    copies.append(pltpu.make_async_copy(spec_in, spec_out, sems.at[1]))
    for copy in copies:
        copy.start()
    for copy in copies:
        copy.wait()


def fused(ne, nb, visit_flux, visit_precision, visit_live, footprint, source_count, spectra_init,
          morphology_init):
    visits, every_blend, bands, block = visit_flux.shape
    owned, slots, pix_part = morphology_init.shape
    ny, nx = factors(ne)
    width = ne * LANES
    chunks = block // width
    per_dest = pix_part // block
    held = per_dest * owned
    hop = max(nx, ny) - 1
    line = max(nx, ny)
    f32 = jnp.float32
    vmem, smem, hbm = (pl.BlockSpec(memory_space=s) for s in (pltpu.VMEM, pltpu.SMEM, pl.ANY))
    dma = pltpu.SemaphoreType.DMA
    parts = pl.pallas_call(
        functools.partial(coadd_kernel, ne=ne, nb=nb, ny=ny, nx=nx),
        out_shape=(
            jax.ShapeDtypeStruct((bands, owned, pix_part), f32),
            jax.ShapeDtypeStruct((bands, owned, slots), f32),
            jax.ShapeDtypeStruct((slots, held, block), f32),
        ),
        in_specs=[hbm, hbm, vmem, hbm, smem, vmem, hbm],
        out_specs=(vmem, vmem, vmem),
        scratch_shapes=[
            pltpu.VMEM((chunks, visits, bands, every_blend, width), visit_flux.dtype),
            pltpu.VMEM((chunks, visits, bands, every_blend, width), visit_precision.dtype),
            pltpu.VMEM((slots, held, block), jnp.int32),
            pltpu.VMEM((bands, held, block), f32),
            pltpu.VMEM((bands, held, block), f32),
            pltpu.VMEM((2, chunks, ne, bands, every_blend, LANES), f32),
            pltpu.VMEM((2, chunks, hop, line, bands, every_blend, LANES), f32),
            pltpu.VMEM((2, chunks, line, bands, every_blend, LANES), f32),
            pltpu.VMEM((2, chunks, hop, bands, every_blend, LANES), f32),
            pltpu.VMEM((chunks, nb, 2, bands, owned, LANES), f32),
            pltpu.VMEM((chunks, 2, bands, per_dest, owned, width), f32),
            pltpu.VMEM((slots, bands, held, LANES), f32),
            pltpu.VMEM((slots, held, LANES), f32),
            pltpu.VMEM((slots, bands + 1, held, LANES), f32),
            pltpu.VMEM((ITERS, ne, held, LANES), f32),
            dma((2, chunks)),
            dma((2, held)),
            dma((2, chunks, hop)),
            dma((2, chunks, hop)),
            dma((2, chunks, hop)),
            dma((2, chunks, hop)),
            dma((chunks, nb)),
            dma((chunks,)),
            dma((ITERS, ne - 1)),
            dma((ITERS, ne - 1)),
        ],
        compiler_params=pltpu.CompilerParams(
            collective_id=0, has_side_effects=True, vmem_limit_bytes=62 * 2**20
        ),
    )(visit_flux.transpose(0, 2, 1, 3), visit_precision.transpose(0, 2, 1, 3), visit_live,
      footprint, source_count, spectra_init.transpose(2, 0, 1), morphology_init)
    coadd, spectra, morphology = pl.pallas_call(
        hand_over,
        out_shape=(
            jax.ShapeDtypeStruct((bands, owned, pix_part), f32),
            jax.ShapeDtypeStruct((bands, owned, slots), f32),
            jax.ShapeDtypeStruct((owned, slots, pix_part), f32),
        ),
        in_specs=[vmem] * 3,
        out_specs=(hbm,) * 3,
        scratch_shapes=[dma((2,)), dma((held,))],
        compiler_params=pltpu.CompilerParams(vmem_limit_bytes=8 * 2**20),
    )(*parts)
    return coadd.transpose(1, 0, 2), spectra.transpose(1, 2, 0), morphology


def on_device(
    visit_flux, visit_precision, visit_live, footprint, source_count, spectra_init, morphology_init
):
    weights = visit_precision.astype(jnp.float32) * visit_live.astype(jnp.float32)[:, :, None, None]
    numerator = jnp.sum(weights * visit_flux.astype(jnp.float32), axis=0)
    weight_sum = jnp.sum(weights, axis=0)
    pix_part = morphology_init.shape[2]
    owned = morphology_init.shape[0]
    numerator, weight_sum = (
        lax.psum_scatter(numerator, "epoch", scatter_dimension=2, tiled=True),
        lax.psum_scatter(weight_sum, "epoch", scatter_dimension=2, tiled=True),
    )
    every_blend, band_count, piece = numerator.shape
    numerator = numerator.reshape(every_blend, band_count, 1, piece)
    weight_sum = weight_sum.reshape(every_blend, band_count, 1, piece)
    numerator, weight_sum = (
        lax.all_to_all(numerator, "blend", split_axis=0, concat_axis=2, tiled=True),
        lax.all_to_all(weight_sum, "blend", split_axis=0, concat_axis=2, tiled=True),
    )
    blocks = numerator.shape[2]
    numerator = numerator.reshape(owned, band_count, blocks, 1, piece)
    weight_sum = weight_sum.reshape(owned, band_count, blocks, 1, piece)
    numerator, weight_sum = (
        lax.all_to_all(numerator, "epoch", split_axis=2, concat_axis=3, tiled=True),
        lax.all_to_all(weight_sum, "epoch", split_axis=2, concat_axis=3, tiled=True),
    )
    numerator = numerator.reshape(owned, band_count, pix_part)
    weight_sum = weight_sum.reshape(owned, band_count, pix_part)
    coadd_flux = numerator / (1.0 + weight_sum)
    coverage = weight_sum / (1.0 + weight_sum)
    slots = footprint.shape[1]
    source_live = (jnp.arange(slots, dtype=jnp.int32)[None, :] < source_count[:, None]).astype(
        jnp.float32
    )
    footprint_mask = footprint.astype(jnp.float32) * source_live[:, :, None]
    live_count = source_count.astype(jnp.float32)
    morphology = morphology_init * footprint_mask
    spectra = spectra_init
    highest = lax.Precision.HIGHEST
    for iteration in range(ITERS):
        blend_model = jnp.einsum("bkc,bkp->bcp", spectra, morphology, precision=highest)
        residual = coverage * (coadd_flux - blend_model)
        morph_grad = jnp.einsum("bkc,bcp->bkp", spectra, residual, precision=highest)
        morph_step = 1.0 / (1.0 + live_count[:, None] * jnp.sum(spectra * spectra, axis=2))
        morphology = (
            jnp.maximum(0.0, morphology + morph_grad * morph_step[:, :, None]) * footprint_mask
        )
        blend_model = jnp.einsum("bkc,bkp->bcp", spectra, morphology, precision=highest)
        residual = coverage * (coadd_flux - blend_model)
        spectra_grad = jnp.einsum("bkp,bcp->bkc", morphology, residual, precision=highest)
        morph_norm = jnp.sum(morphology * morphology, axis=2)
        spectra_grad, morph_norm = lax.psum((spectra_grad, morph_norm), "epoch")
        spectra = jnp.maximum(
            0.0, spectra + spectra_grad / (1.0 + live_count[:, None] * morph_norm)[:, :, None]
        )
    return (coadd_flux, spectra, morphology)


def solution(mesh):
    ne, nb = mesh.shape["epoch"], mesh.shape["blend"]

    def step(visit_flux, visit_precision, visit_live, footprint, source_count, spectra_init,
             morphology_init):
        block, bands = visit_flux.shape[3], visit_flux.shape[2]
        owned, pix_part = morphology_init.shape[0], morphology_init.shape[2]
        ny, nx = factors(ne)
        fits = (
            block % (ne * LANES) == 0
            and pix_part % block == 0
            and min(ny, nx) > 1
            and morphology_init.shape[1] * (bands + 1) <= LANES
        )
        run = functools.partial(fused, ne, nb) if fits else on_device
        return run(visit_flux, visit_precision, visit_live, footprint, source_count, spectra_init,
                   morphology_init)

    in_specs = (
        P("epoch", None, None, "blend"),
        P("epoch", None, None, "blend"),
        P("epoch", None),
        P("blend", None, "epoch"),
        P("blend"),
        P("blend", None, None),
        P("blend", None, "epoch"),
    )
    out_specs = (P("blend", None, "epoch"), P("blend", None, None), P("blend", None, "epoch"))
    return jax.shard_map(
        step, mesh=mesh, in_specs=in_specs, out_specs=out_specs, check_vma=False
    )
```

```python
import functools

import jax
import jax.numpy as jnp
from jax import lax
from jax.experimental import pallas as pl
from jax.experimental.pallas import tpu as pltpu
from jax.sharding import PartitionSpec as P

ITERS = 2
AHEAD = 3


LANES = 128
MESH = pl.DeviceIdType.MESH


def factors(count):
    rows = max(d for d in range(1, count + 1) if count % d == 0 and d * d <= count)
    return rows, count // rows


def coadd_kernel(
    flux_hbm, prec_hbm, live_ref, foot_hbm, count_ref, spec_ref, morph_hbm,
    coadd_ref, spec_out, morph_ref,
    flux_v, prec_v, foot_v, flux_c, cover,
    stage, land1, part, land2, final, column, pieces, spectra, step_ref, acc, sums,
    in_sem, side_sem, s1_send, s1_recv, s2_send, s2_recv, s3_send, s3_recv, s4_send, s4_recv, ps_send, ps_recv,
    *, ne, nb, ny, nx,
):
    visits, bands, every_blend, block = flux_hbm.shape
    owned, slots, pix_part = morph_hbm.shape
    chunks = flux_v.shape[0]
    width = block // chunks
    per_dest = pix_part // block
    held = per_dest * owned
    cuts = final.shape[0] // chunks
    some = bands // cuts
    units = chunks * cuts
    e = lax.axis_index("epoch")
    j = lax.axis_index("blend")
    y, x = e // nx, e % nx
    f32 = jnp.float32

    def in_copy(q):
        window = pl.ds(q * width, width)
        return (
            pltpu.make_async_copy(prec_hbm.at[:, :, :, window], prec_v.at[q], in_sem.at[0, q]),
            pltpu.make_async_copy(flux_hbm.at[:, :, :, window], flux_v.at[q], in_sem.at[1, q]),
        )

    side = []
    for s in range(per_dest):
        for b in range(owned):
            row = s * owned + b
            window = pl.ds(s * block, block)
            side.append(pltpu.make_async_copy(
                foot_hbm.at[b, :, window], foot_v.at[:, row, :], side_sem.at[0, row]))
            side.append(pltpu.make_async_copy(
                morph_hbm.at[b, :, window], morph_ref.at[:, row, :], side_sem.at[1, row]))

    for q in range(chunks):
        for copy in in_copy(q):
            copy.start()

    barrier = pltpu.get_barrier_semaphore()
    total = ne * nb
    mine = e * nb + j

    def greet(d, carry):
        other = lax.rem(mine + d, total)
        pl.semaphore_signal(
            barrier, inc=1, device_id=(other // nb, lax.rem(other, nb)), device_id_type=MESH
        )
        return carry

    lax.fori_loop(1, total, greet, 0)

    square_r = lax.broadcasted_iota(jnp.int32, (every_blend, every_blend), 0)
    square_c = lax.broadcasted_iota(jnp.int32, (every_blend, every_blend), 1)
    lives = []
    for v in range(visits):
        row = jnp.broadcast_to(live_ref[v : v + 1, :].astype(f32), (every_blend, every_blend))
        tall = jnp.sum(jnp.where(square_r == square_c, row, 0.0), axis=1, keepdims=True)
        lives.append(jnp.broadcast_to(tall, (every_blend, LANES)))

    def split(u):
        return u // cuts, pl.ds(u % cuts * some, some)

    def local_sum(u):
        q, h = u // cuts, u % cuts
        if h == 0:
            for copy in in_copy(q):
                copy.wait()

        def one(c, carry):
            for p in range(ne):
                lanes = slice(p * LANES, (p + 1) * LANES)
                py, px = p // nx, p % nx
                num = None
                for v in range(visits):
                    w = prec_v[q, v, c, :, lanes].astype(f32) * lives[v]
                    n = w * flux_v[q, v, c, :, lanes].astype(f32)
                    num, wsum = (n, w) if num is None else (num + n, wsum + w)
                stage[0, q, px * ny + py, c] = num
                stage[1, q, py * nx + px, c] = wsum
            return carry

        lax.fori_loop(h * some, (h + 1) * some, one, 0)

    def line(a, first):
        along_x = (a == 0) == first
        return (x, nx) if along_x else (y, ny)

    def device_at(a, first, where):
        along_x = (a == 0) == first
        return (y * nx + where if along_x else where * nx + x, j)

    def s1(a, u, d):
        q, some_bands = split(u)
        at, n = line(a, True)
        other = line(a, False)[1]
        to = lax.rem(at + d, n)
        return pltpu.make_async_remote_copy(
            src_ref=stage.at[a, q, pl.ds(to * other, other), some_bands],
            dst_ref=land1.at[a, q, d - 1, pl.ds(0, other), some_bands],
            send_sem=s1_send.at[a, u, d - 1], recv_sem=s1_recv.at[a, u, d - 1],
            device_id=device_at(a, True, to), device_id_type=MESH,
        )

    def s2(a, u, d):
        q, some_bands = split(u)
        at, n = line(a, False)
        to = lax.rem(at + d, n)
        return pltpu.make_async_remote_copy(
            src_ref=part.at[a, q, to, some_bands],
            dst_ref=land2.at[a, q, d - 1, some_bands],
            send_sem=s2_send.at[a, u, d - 1], recv_sem=s2_recv.at[a, u, d - 1],
            device_id=device_at(a, False, to), device_id_type=MESH,
        )

    def s1_start(u):
        for a in range(2):
            for d in range(1, line(a, True)[1]):
                s1(a, u, d).start()

    def s2_start(u):
        q, h = u // cuts, u % cuts
        for a in range(2):
            at, n = line(a, True)
            others = line(a, False)[1]
            for d in range(1, n):
                s1(a, u, d).wait_recv()

            def add(c, carry):
                for o in range(others):
                    v = stage[a, q, at * others + o, c]
                    for d in range(1, n):
                        v = v + land1[a, q, d - 1, o, c]
                    part[a, q, o, c] = v
                return carry

            lax.fori_loop(h * some, (h + 1) * some, add, 0)
            for d in range(1, others):
                s2(a, u, d).start()

    def s3(u, d):
        to = lax.rem(j + d, nb)
        return pltpu.make_async_remote_copy(
            src_ref=final.at[u, to], dst_ref=column.at[u, j],
            send_sem=s3_send.at[u, d - 1], recv_sem=s3_recv.at[u, d - 1],
            device_id=(e, to), device_id_type=MESH,
        )

    def s3_own(u):
        return pltpu.make_async_copy(final.at[u, j], column.at[u, j], s3_send.at[u, nb - 1])

    def s3_start(u):
        q, h = u // cuts, u % cuts
        for a in range(2):
            at, n = line(a, False)
            for d in range(1, n):
                s2(a, u, d).wait_recv()

            def add(i, carry):
                c = h * some + i
                v = part[a, q, at, c]
                for d in range(1, n):
                    v = v + land2[a, q, d - 1, c]
                for to in range(nb):
                    final[u, to, a, i] = v[to * owned : (to + 1) * owned, :]
                return carry

            lax.fori_loop(0, some, add, 0)
        s3_own(u).start()
        for d in range(1, nb):
            s3(u, d).start()

    def s4(u, d):
        to = lax.rem(e + d, ne)
        return pltpu.make_async_remote_copy(
            src_ref=column.at[u, pl.ds(to * per_dest, per_dest)], dst_ref=pieces.at[u, e],
            send_sem=s4_send.at[u, d - 1], recv_sem=s4_recv.at[u, d - 1],
            device_id=(to, j), device_id_type=MESH,
        )

    def s4_own(u):
        return pltpu.make_async_copy(
            column.at[u, pl.ds(e * per_dest, per_dest)], pieces.at[u, e], s4_send.at[u, ne - 1]
        )

    def s4_start(u):
        s3_own(u).wait()
        for d in range(1, nb):
            s3(u, d).wait_recv()
        for d in range(ne - 1, 0, -1):
            s4(u, d).start()
        s4_own(u).start()

    sub = lax.broadcasted_iota(jnp.int32, (held, LANES), 0)
    lane = lax.broadcasted_iota(jnp.int32, (held, LANES), 1)
    count = jnp.zeros((held, LANES), jnp.int32)
    for b in range(owned):
        count = jnp.where(lax.rem(sub, owned) == b, count_ref[b], count)
    live_count = count.astype(f32)

    def steps():
        for k in range(slots):
            norm = None
            for c in range(bands):
                s = spectra[k, c]
                norm = s * s if norm is None else norm + s * s
            step_ref[k] = 1.0 / (1.0 + live_count * norm)

    group = 2

    def deblend(start, first):
        runs = [
            pl.ds(pl.multiple_of(start + t * LANES, LANES), LANES) for t in range(group)
        ]

        def masks(k):
            live = jnp.where(count > k, 1.0, 0.0).astype(f32)
            return [foot_v[k, :, px].astype(f32) * live for px in runs]

        def residual(morph):
            res = []
            for c in range(bands):
                model = [None] * group
                for k in range(slots):
                    s = spectra[k, c]
                    for t in range(group):
                        v = s * morph[k][t]
                        model[t] = v if k == 0 else model[t] + v
                res.append([
                    cover[c, :, px] * (flux_c[c, :, px] - model[t]) for t, px in enumerate(runs)
                ])
            return res

        morph = []
        for k in range(slots):
            m = [morph_ref[k, :, px] for px in runs]
            morph.append([a * b for a, b in zip(m, masks(k))] if first else m)
        res = residual(morph)
        for k in range(slots):
            mask = masks(k)
            grad = [None] * group
            for c in range(bands):
                s = spectra[k, c]
                for t in range(group):
                    v = s * res[c][t]
                    grad[t] = v if c == 0 else grad[t] + v
            step = step_ref[k]
            for t, px in enumerate(runs):
                m = jnp.maximum(0.0, morph[k][t] + grad[t] * step) * mask[t]
                morph[k][t] = m
                morph_ref[k, :, px] = m
        res = residual(morph)
        for k in range(slots):
            for c in range(bands):
                v = acc[k, c]
                for t in range(group):
                    v = v + morph[k][t] * res[c][t]
                acc[k, c] = v
            v = acc[k, bands]
            for t in range(group):
                v = v + morph[k][t] * morph[k][t]
            acc[k, bands] = v

    def finish(q):
        for h in range(cuts):
            u = q * cuts + h
            s4_own(u).wait()
            for d in range(1, ne):
                s4(u, d).wait_recv()

            def unpack(i, carry, u=u, h=h):
                c = h * some + i
                for p in range(ne):
                    at = q * width + p * LANES
                    for s in range(per_dest):
                        rows = slice(s * owned, (s + 1) * owned)
                        wsum = pieces[u, p, s, 1, i]
                        inv = 1.0 / (1.0 + wsum)
                        flux = pieces[u, p, s, 0, i] * inv
                        coadd_ref[c, :, s * block + at : s * block + at + LANES] = flux
                        flux_c[c, rows, at : at + LANES] = flux
                        cover[c, rows, at : at + LANES] = wsum * inv
                return carry

            lax.fori_loop(0, some, unpack, 0)

        def go(i, carry):
            deblend(q * width + i * (group * LANES), True)
            return carry

        lax.fori_loop(0, width // (group * LANES), go, 0)

    def ps_copy(it, d):
        to = lax.rem(e + d, ne)
        return pltpu.make_async_remote_copy(
            src_ref=sums.at[it, 0], dst_ref=sums.at[it, d],
            send_sem=ps_send.at[it, d - 1], recv_sem=ps_recv.at[it, d - 1],
            device_id=(to, j), device_id_type=MESH,
        )

    def update(it):
        packed = jnp.zeros((held, LANES), f32)
        for k in range(slots):
            for c in range(bands + 1):
                whole = jnp.sum(acc[k, c], axis=1, keepdims=True)
                packed = jnp.where(lane == k * (bands + 1) + c, whole, packed)
        sums[it, 0] = packed
        for d in range(1, ne):
            ps_copy(it, d).start()
        for d in range(1, ne):
            ps_copy(it, d).wait_recv()
        whole = None
        for o in range(ne):
            v = sums[it, lax.rem(e - o + ne, ne)]
            whole = v if whole is None else whole + v
        one = whole[0:owned, :]
        for s in range(1, per_dest):
            one = one + whole[s * owned : (s + 1) * owned, :]
        whole = jnp.concatenate([one] * per_dest, axis=0)
        for k in range(slots):
            at = k * (bands + 1)
            norm = jnp.broadcast_to(whole[:, at + bands : at + bands + 1], (held, LANES))
            scale = 1.0 / (1.0 + live_count * norm)
            for c in range(bands):
                grad = jnp.broadcast_to(whole[:, at + c : at + c + 1], (held, LANES))
                spectra[k, c] = jnp.maximum(0.0, spectra[k, c] + grad * scale)

    local_sum(0)
    pl.semaphore_wait(barrier, total - 1)
    s1_start(0)
    for u in range(1, min(AHEAD, units)):
        local_sum(u)
        s1_start(u)
    for copy in side:
        copy.start()

    acc[...] = jnp.zeros_like(acc)
    for k in range(slots):
        for c in range(bands):
            start = jnp.broadcast_to(spec_ref[c, :, k : k + 1], (owned, LANES))
            spectra[k, c] = jnp.concatenate([start] * per_dest, axis=0)
    steps()

    for u in range(units + 3):
        if u < units:
            s2_start(u)
        if u + AHEAD < units:
            local_sum(u + AHEAD)
            s1_start(u + AHEAD)
        if 0 <= u - 1 < units:
            s3_start(u - 1)
        if 0 <= u - 2 < units:
            s4_start(u - 2)
        if u == 3:
            for copy in side:
                copy.wait()
        if 0 <= u - 3 < units and (u - 3) % cuts == cuts - 1:
            finish((u - 3) // cuts)

    update(0)
    for it in range(1, ITERS):
        steps()
        acc[...] = jnp.zeros_like(acc)

        def again(i, carry):
            deblend(i * (group * LANES), False)
            return carry

        lax.fori_loop(0, block // (group * LANES), again, 0)
        update(it)
    for c in range(bands):
        out = spectra[0, c]
        for k in range(1, slots):
            out = jnp.where(lane == k, spectra[k, c], out)
        spec_out[c] = out[0:owned, :slots]

    for u in range(units):
        for a in range(2):
            for d in range(1, line(a, True)[1]):
                s1(a, u, d).wait_send()
            for d in range(1, line(a, False)[1]):
                s2(a, u, d).wait_send()
        for d in range(1, nb):
            s3(u, d).wait_send()
        for d in range(1, ne):
            s4(u, d).wait_send()
    for it in range(ITERS):
        for d in range(1, ne):
            ps_copy(it, d).wait_send()


def hand_over(coadd_in, spec_in, morph_in, coadd_out, spec_out, morph_out, sems, row_sems):
    owned, _, pix_part = morph_out.shape
    _, held, block = morph_in.shape
    copies = [
        pltpu.make_async_copy(morph_in.at[:, row, :],
                              morph_out.at[row % owned, :, pl.ds(row // owned * block, block)],
                              row_sems.at[row])
        for row in range(held)
    ]
    copies.append(pltpu.make_async_copy(coadd_in, coadd_out, sems.at[0]))
    copies.append(pltpu.make_async_copy(spec_in, spec_out, sems.at[1]))
    for copy in copies:
        copy.start()
    for copy in copies:
        copy.wait()


def fused(ne, nb, visit_flux, visit_precision, visit_live, footprint, source_count, spectra_init,
          morphology_init):
    visits, every_blend, bands, block = visit_flux.shape
    owned, slots, pix_part = morphology_init.shape
    ny, nx = factors(ne)
    width = ne * LANES
    chunks = block // width
    per_dest = pix_part // block
    held = per_dest * owned
    hop = max(nx, ny) - 1
    line = max(nx, ny)
    cuts = 2 if bands % 2 == 0 else 1
    units, some = chunks * cuts, bands // cuts
    f32 = jnp.float32
    vmem, smem, hbm = (pl.BlockSpec(memory_space=s) for s in (pltpu.VMEM, pltpu.SMEM, pl.ANY))
    dma = pltpu.SemaphoreType.DMA
    parts = pl.pallas_call(
        functools.partial(coadd_kernel, ne=ne, nb=nb, ny=ny, nx=nx),
        out_shape=(
            jax.ShapeDtypeStruct((bands, owned, pix_part), f32),
            jax.ShapeDtypeStruct((bands, owned, slots), f32),
            jax.ShapeDtypeStruct((slots, held, block), f32),
        ),
        in_specs=[hbm, hbm, vmem, hbm, smem, vmem, hbm],
        out_specs=(vmem, vmem, vmem),
        scratch_shapes=[
            pltpu.VMEM((chunks, visits, bands, every_blend, width), visit_flux.dtype),
            pltpu.VMEM((chunks, visits, bands, every_blend, width), visit_precision.dtype),
            pltpu.VMEM((slots, held, block), jnp.int32),
            pltpu.VMEM((bands, held, block), f32),
            pltpu.VMEM((bands, held, block), f32),
            pltpu.VMEM((2, chunks, ne, bands, every_blend, LANES), f32),
            pltpu.VMEM((2, chunks, hop, line, bands, every_blend, LANES), f32),
            pltpu.VMEM((2, chunks, line, bands, every_blend, LANES), f32),
            pltpu.VMEM((2, chunks, hop, bands, every_blend, LANES), f32),
            pltpu.VMEM((units, nb, 2, some, owned, LANES), f32),
            pltpu.VMEM((units, nb, 2, some, owned, LANES), f32),
            pltpu.VMEM((units, ne, per_dest, 2, some, owned, LANES), f32),
            pltpu.VMEM((slots, bands, held, LANES), f32),
            pltpu.VMEM((slots, held, LANES), f32),
            pltpu.VMEM((slots, bands + 1, held, LANES), f32),
            pltpu.VMEM((ITERS, ne, held, LANES), f32),
            dma((2, chunks)),
            dma((2, held)),
            dma((2, units, hop)),
            dma((2, units, hop)),
            dma((2, units, hop)),
            dma((2, units, hop)),
            dma((units, nb)),
            dma((units, nb - 1)),
            dma((units, ne)),
            dma((units, ne - 1)),
            dma((ITERS, ne - 1)),
            dma((ITERS, ne - 1)),
        ],
        compiler_params=pltpu.CompilerParams(
            collective_id=0, has_side_effects=True, vmem_limit_bytes=58 * 2**20
        ),
    )(visit_flux.transpose(0, 2, 1, 3), visit_precision.transpose(0, 2, 1, 3), visit_live,
      footprint, source_count, spectra_init.transpose(2, 0, 1), morphology_init)
    coadd, spectra, morphology = pl.pallas_call(
        hand_over,
        out_shape=(
            jax.ShapeDtypeStruct((bands, owned, pix_part), f32),
            jax.ShapeDtypeStruct((bands, owned, slots), f32),
            jax.ShapeDtypeStruct((owned, slots, pix_part), f32),
        ),
        in_specs=[vmem] * 3,
        out_specs=(hbm,) * 3,
        scratch_shapes=[dma((2,)), dma((held,))],
        compiler_params=pltpu.CompilerParams(vmem_limit_bytes=8 * 2**20),
    )(*parts)
    return coadd.transpose(1, 0, 2), spectra.transpose(1, 2, 0), morphology


def on_device(
    visit_flux, visit_precision, visit_live, footprint, source_count, spectra_init, morphology_init
):
    weights = visit_precision.astype(jnp.float32) * visit_live.astype(jnp.float32)[:, :, None, None]
    numerator = jnp.sum(weights * visit_flux.astype(jnp.float32), axis=0)
    weight_sum = jnp.sum(weights, axis=0)
    pix_part = morphology_init.shape[2]
    owned = morphology_init.shape[0]
    numerator, weight_sum = (
        lax.psum_scatter(numerator, "epoch", scatter_dimension=2, tiled=True),
        lax.psum_scatter(weight_sum, "epoch", scatter_dimension=2, tiled=True),
    )
    every_blend, band_count, piece = numerator.shape
    numerator = numerator.reshape(every_blend, band_count, 1, piece)
    weight_sum = weight_sum.reshape(every_blend, band_count, 1, piece)
    numerator, weight_sum = (
        lax.all_to_all(numerator, "blend", split_axis=0, concat_axis=2, tiled=True),
        lax.all_to_all(weight_sum, "blend", split_axis=0, concat_axis=2, tiled=True),
    )
    blocks = numerator.shape[2]
    numerator = numerator.reshape(owned, band_count, blocks, 1, piece)
    weight_sum = weight_sum.reshape(owned, band_count, blocks, 1, piece)
    numerator, weight_sum = (
        lax.all_to_all(numerator, "epoch", split_axis=2, concat_axis=3, tiled=True),
        lax.all_to_all(weight_sum, "epoch", split_axis=2, concat_axis=3, tiled=True),
    )
    numerator = numerator.reshape(owned, band_count, pix_part)
    weight_sum = weight_sum.reshape(owned, band_count, pix_part)
    coadd_flux = numerator / (1.0 + weight_sum)
    coverage = weight_sum / (1.0 + weight_sum)
    slots = footprint.shape[1]
    source_live = (jnp.arange(slots, dtype=jnp.int32)[None, :] < source_count[:, None]).astype(
        jnp.float32
    )
    footprint_mask = footprint.astype(jnp.float32) * source_live[:, :, None]
    live_count = source_count.astype(jnp.float32)
    morphology = morphology_init * footprint_mask
    spectra = spectra_init
    highest = lax.Precision.HIGHEST
    for iteration in range(ITERS):
        blend_model = jnp.einsum("bkc,bkp->bcp", spectra, morphology, precision=highest)
        residual = coverage * (coadd_flux - blend_model)
        morph_grad = jnp.einsum("bkc,bcp->bkp", spectra, residual, precision=highest)
        morph_step = 1.0 / (1.0 + live_count[:, None] * jnp.sum(spectra * spectra, axis=2))
        morphology = (
            jnp.maximum(0.0, morphology + morph_grad * morph_step[:, :, None]) * footprint_mask
        )
        blend_model = jnp.einsum("bkc,bkp->bcp", spectra, morphology, precision=highest)
        residual = coverage * (coadd_flux - blend_model)
        spectra_grad = jnp.einsum("bkp,bcp->bkc", morphology, residual, precision=highest)
        morph_norm = jnp.sum(morphology * morphology, axis=2)
        spectra_grad, morph_norm = lax.psum((spectra_grad, morph_norm), "epoch")
        spectra = jnp.maximum(
            0.0, spectra + spectra_grad / (1.0 + live_count[:, None] * morph_norm)[:, :, None]
        )
    return (coadd_flux, spectra, morphology)


def solution(mesh):
    ne, nb = mesh.shape["epoch"], mesh.shape["blend"]

    def step(visit_flux, visit_precision, visit_live, footprint, source_count, spectra_init,
             morphology_init):
        block, bands = visit_flux.shape[3], visit_flux.shape[2]
        owned, pix_part = morphology_init.shape[0], morphology_init.shape[2]
        ny, nx = factors(ne)
        fits = (
            block % (ne * LANES) == 0
            and pix_part % block == 0
            and min(ny, nx) > 1
            and morphology_init.shape[1] * (bands + 1) <= LANES
        )
        run = functools.partial(fused, ne, nb) if fits else on_device
        return run(visit_flux, visit_precision, visit_live, footprint, source_count, spectra_init,
                   morphology_init)

    in_specs = (
        P("epoch", None, None, "blend"),
        P("epoch", None, None, "blend"),
        P("epoch", None),
        P("blend", None, "epoch"),
        P("blend"),
        P("blend", None, None),
        P("blend", None, "epoch"),
    )
    out_specs = (P("blend", None, "epoch"), P("blend", None, None), P("blend", None, "epoch"))
    return jax.shard_map(
        step, mesh=mesh, in_specs=in_specs, out_specs=out_specs, check_vma=False
    )
```

```python
import functools

import jax
import jax.numpy as jnp
from jax import lax
from jax.experimental import pallas as pl
from jax.experimental.pallas import tpu as pltpu
from jax.sharding import PartitionSpec as P

ITERS = 2


LANES = 128
MESH = pl.DeviceIdType.MESH


def factors(count):
    rows = max(d for d in range(1, count + 1) if count % d == 0 and d * d <= count)
    return rows, count // rows


def coadd_kernel(
    flux_hbm, prec_hbm, live_ref, foot_hbm, count_ref, spec_ref, morph_hbm,
    coadd_ref, spec_out, morph_ref,
    flux_v, prec_v, foot_v, flux_c, cover,
    stage, land1, part, land2, final, pieces, spectra, step_ref, acc, sums,
    in_sem, side_sem, s1_send, s1_recv, s2_send, s2_recv, s3_send, s3_recv, ps_send, ps_recv,
    *, ne, nb, ny, nx,
):
    visits, bands, every_blend, block = flux_hbm.shape
    owned, slots, pix_part = morph_hbm.shape
    chunks = flux_v.shape[0]
    width = block // chunks
    per_dest = pix_part // block
    held = per_dest * owned
    e = lax.axis_index("epoch")
    j = lax.axis_index("blend")
    y, x = e // nx, e % nx
    home_e = j // per_dest
    home_slot = j % per_dest
    f32 = jnp.float32

    def in_copy(q):
        window = pl.ds(q * width, width)
        return (
            pltpu.make_async_copy(prec_hbm.at[:, :, :, window], prec_v.at[q], in_sem.at[0, q]),
            pltpu.make_async_copy(flux_hbm.at[:, :, :, window], flux_v.at[q], in_sem.at[1, q]),
        )

    side = []
    for s in range(per_dest):
        for b in range(owned):
            row = s * owned + b
            window = pl.ds(s * block, block)
            side.append(pltpu.make_async_copy(
                foot_hbm.at[b, :, window], foot_v.at[:, row, :], side_sem.at[0, row]))
            side.append(pltpu.make_async_copy(
                morph_hbm.at[b, :, window], morph_ref.at[:, row, :], side_sem.at[1, row]))

    for q in range(chunks):
        for copy in in_copy(q):
            copy.start()

    barrier = pltpu.get_barrier_semaphore()
    total = ne * nb
    mine = e * nb + j

    def greet(d, carry):
        other = lax.rem(mine + d, total)
        pl.semaphore_signal(
            barrier, inc=1, device_id=(other // nb, lax.rem(other, nb)), device_id_type=MESH
        )
        return carry

    lax.fori_loop(1, total, greet, 0)

    square_r = lax.broadcasted_iota(jnp.int32, (every_blend, every_blend), 0)
    square_c = lax.broadcasted_iota(jnp.int32, (every_blend, every_blend), 1)
    lives = []
    for v in range(visits):
        row = jnp.broadcast_to(live_ref[v : v + 1, :].astype(f32), (every_blend, every_blend))
        column = jnp.sum(jnp.where(square_r == square_c, row, 0.0), axis=1, keepdims=True)
        lives.append(jnp.broadcast_to(column, (every_blend, LANES)))

    def local_sum(q):
        for copy in in_copy(q):
            copy.wait()

        def one(c, carry):
            for p in range(ne):
                lanes = slice(p * LANES, (p + 1) * LANES)
                py, px = p // nx, p % nx
                num = None
                for v in range(visits):
                    w = prec_v[q, v, c, :, lanes].astype(f32) * lives[v]
                    n = w * flux_v[q, v, c, :, lanes].astype(f32)
                    num, wsum = (n, w) if num is None else (num + n, wsum + w)
                stage[0, q, px * ny + py, c] = num
                stage[1, q, py * nx + px, c] = wsum
            return carry

        lax.fori_loop(0, bands, one, 0)

    def line(a, first):
        along_x = (a == 0) == first
        return (x, nx) if along_x else (y, ny)

    def device_at(a, first, where):
        along_x = (a == 0) == first
        return (y * nx + where if along_x else where * nx + x, j)

    def s1(a, q, d):
        at, n = line(a, True)
        other = line(a, False)[1]
        to = lax.rem(at + d, n)
        return pltpu.make_async_remote_copy(
            src_ref=stage.at[a, q, pl.ds(to * other, other)],
            dst_ref=land1.at[a, q, d - 1],
            send_sem=s1_send.at[a, q, d - 1], recv_sem=s1_recv.at[a, q, d - 1],
            device_id=device_at(a, True, to), device_id_type=MESH,
        )

    def s2(a, q, d):
        at, n = line(a, False)
        to = lax.rem(at + d, n)
        return pltpu.make_async_remote_copy(
            src_ref=part.at[a, q, to],
            dst_ref=land2.at[a, q, d - 1],
            send_sem=s2_send.at[a, q, d - 1], recv_sem=s2_recv.at[a, q, d - 1],
            device_id=device_at(a, False, to), device_id_type=MESH,
        )

    def s1_start(q):
        for a in range(2):
            for d in range(1, line(a, True)[1]):
                s1(a, q, d).start()

    def s2_start(q):
        for a in range(2):
            at, n = line(a, True)
            others = line(a, False)[1]
            for d in range(1, n):
                s1(a, q, d).wait_recv()

            def add(c, carry):
                for o in range(others):
                    v = stage[a, q, at * others + o, c]
                    for d in range(1, n):
                        v = v + land1[a, q, d - 1, o, c]
                    part[a, q, o, c] = v
                return carry

            lax.fori_loop(0, bands, add, 0)
            for d in range(1, others):
                s2(a, q, d).start()

    here = home_e == e

    def landing(q):
        lanes = pl.ds(pl.multiple_of(e * LANES, LANES), LANES)
        return pieces.at[q, :, :, home_slot, :, lanes]

    def s3_local(q):
        return pltpu.make_async_copy(final.at[q, j], landing(q), s3_recv.at[q])

    def s3_remote(q, to):
        return pltpu.make_async_remote_copy(
            src_ref=final.at[q, to], dst_ref=landing(q),
            send_sem=s3_send.at[q, to], recv_sem=s3_recv.at[q],
            device_id=(home_e, to), device_id_type=MESH,
        )

    def s3_start(q):
        for a in range(2):
            at, n = line(a, False)
            for d in range(1, n):
                s2(a, q, d).wait_recv()

            def add(c, carry):
                v = part[a, q, at, c]
                for d in range(1, n):
                    v = v + land2[a, q, d - 1, c]
                for to in range(nb):
                    final[q, to, a, c] = v[to * owned : (to + 1) * owned, :]
                return carry

            lax.fori_loop(0, bands, add, 0)

        def send(d, carry):
            s3_remote(q, lax.rem(j + d, nb)).start()
            return carry

        lax.fori_loop(1, nb, send, 0)

        @pl.when(here)
        def _():
            s3_local(q).start()

        @pl.when(jnp.logical_not(here))
        def _():
            s3_remote(q, j).start()

    sub = lax.broadcasted_iota(jnp.int32, (held, LANES), 0)
    lane = lax.broadcasted_iota(jnp.int32, (held, LANES), 1)
    count = jnp.zeros((held, LANES), jnp.int32)
    for b in range(owned):
        count = jnp.where(lax.rem(sub, owned) == b, count_ref[b], count)
    live_count = count.astype(f32)

    def steps():
        for k in range(slots):
            norm = None
            for c in range(bands):
                s = spectra[k, c]
                norm = s * s if norm is None else norm + s * s
            step_ref[k] = 1.0 / (1.0 + live_count * norm)

    group = 2

    def deblend(start, first):
        runs = [
            pl.ds(pl.multiple_of(start + t * LANES, LANES), LANES) for t in range(group)
        ]

        def masks(k):
            live = jnp.where(count > k, 1.0, 0.0).astype(f32)
            return [foot_v[k, :, px].astype(f32) * live for px in runs]

        def residual(morph):
            res = []
            for c in range(bands):
                model = [None] * group
                for k in range(slots):
                    s = spectra[k, c]
                    for t in range(group):
                        v = s * morph[k][t]
                        model[t] = v if k == 0 else model[t] + v
                res.append([
                    cover[c, :, px] * (flux_c[c, :, px] - model[t]) for t, px in enumerate(runs)
                ])
            return res

        morph = []
        for k in range(slots):
            m = [morph_ref[k, :, px] for px in runs]
            morph.append([a * b for a, b in zip(m, masks(k))] if first else m)
        res = residual(morph)
        for k in range(slots):
            mask = masks(k)
            grad = [None] * group
            for c in range(bands):
                s = spectra[k, c]
                for t in range(group):
                    v = s * res[c][t]
                    grad[t] = v if c == 0 else grad[t] + v
            step = step_ref[k]
            for t, px in enumerate(runs):
                m = jnp.maximum(0.0, morph[k][t] + grad[t] * step) * mask[t]
                morph[k][t] = m
                morph_ref[k, :, px] = m
        res = residual(morph)
        for k in range(slots):
            for c in range(bands):
                v = acc[k, c]
                for t in range(group):
                    v = v + morph[k][t] * res[c][t]
                acc[k, c] = v
            v = acc[k, bands]
            for t in range(group):
                v = v + morph[k][t] * morph[k][t]
            acc[k, bands] = v

    def finish(q):
        pltpu.make_async_copy(pieces.at[q], pieces.at[q], s3_recv.at[q]).wait()
        at = slice(q * width, (q + 1) * width)

        def unpack(c, carry):
            for s in range(per_dest):
                rows = slice(s * owned, (s + 1) * owned)
                wsum = pieces[q, 1, c, s]
                inv = 1.0 / (1.0 + wsum)
                flux = pieces[q, 0, c, s] * inv
                coadd_ref[c, :, s * block + q * width : s * block + (q + 1) * width] = flux
                flux_c[c, rows, at] = flux
                cover[c, rows, at] = wsum * inv
            return carry

        lax.fori_loop(0, bands, unpack, 0)

        def go(i, carry):
            deblend(q * width + i * (group * LANES), True)
            return carry

        lax.fori_loop(0, width // (group * LANES), go, 0)

    def ps_copy(it, d):
        to = lax.rem(e + d, ne)
        return pltpu.make_async_remote_copy(
            src_ref=sums.at[it, 0], dst_ref=sums.at[it, d],
            send_sem=ps_send.at[it, d - 1], recv_sem=ps_recv.at[it, d - 1],
            device_id=(to, j), device_id_type=MESH,
        )

    def update(it):
        packed = jnp.zeros((held, LANES), f32)
        for k in range(slots):
            for c in range(bands + 1):
                whole = jnp.sum(acc[k, c], axis=1, keepdims=True)
                packed = jnp.where(lane == k * (bands + 1) + c, whole, packed)
        sums[it, 0] = packed
        for d in range(1, ne):
            ps_copy(it, d).start()
        for d in range(1, ne):
            ps_copy(it, d).wait_recv()
        whole = None
        for o in range(ne):
            v = sums[it, lax.rem(e - o + ne, ne)]
            whole = v if whole is None else whole + v
        one = whole[0:owned, :]
        for s in range(1, per_dest):
            one = one + whole[s * owned : (s + 1) * owned, :]
        whole = jnp.concatenate([one] * per_dest, axis=0)
        for k in range(slots):
            at = k * (bands + 1)
            norm = jnp.broadcast_to(whole[:, at + bands : at + bands + 1], (held, LANES))
            scale = 1.0 / (1.0 + live_count * norm)
            for c in range(bands):
                grad = jnp.broadcast_to(whole[:, at + c : at + c + 1], (held, LANES))
                spectra[k, c] = jnp.maximum(0.0, spectra[k, c] + grad * scale)

    local_sum(0)
    pl.semaphore_wait(barrier, total - 1)
    s1_start(0)
    if chunks > 1:
        local_sum(1)
        s1_start(1)
    for copy in side:
        copy.start()

    acc[...] = jnp.zeros_like(acc)
    for k in range(slots):
        for c in range(bands):
            start = jnp.broadcast_to(spec_ref[c, :, k : k + 1], (owned, LANES))
            spectra[k, c] = jnp.concatenate([start] * per_dest, axis=0)
    steps()

    for q in range(chunks + 2):
        if q < chunks:
            s2_start(q)
        if q + 2 < chunks:
            local_sum(q + 2)
            s1_start(q + 2)
        if 0 <= q - 1 < chunks:
            s3_start(q - 1)
        if q == 2:
            for copy in side:
                copy.wait()
        if 0 <= q - 2 < chunks:
            finish(q - 2)

    update(0)
    for it in range(1, ITERS):
        steps()
        acc[...] = jnp.zeros_like(acc)

        def again(i, carry):
            deblend(i * (group * LANES), False)
            return carry

        lax.fori_loop(0, block // (group * LANES), again, 0)
        update(it)
    for c in range(bands):
        out = spectra[0, c]
        for k in range(1, slots):
            out = jnp.where(lane == k, spectra[k, c], out)
        spec_out[c] = out[0:owned, :slots]

    for q in range(chunks):
        for a in range(2):
            for d in range(1, line(a, True)[1]):
                s1(a, q, d).wait_send()
            for d in range(1, line(a, False)[1]):
                s2(a, q, d).wait_send()

        def sent(d, carry, q=q):
            s3_remote(q, lax.rem(j + d, nb)).wait_send()
            return carry

        lax.fori_loop(1, nb, sent, 0)

        @pl.when(jnp.logical_not(here))
        def _(q=q):
            s3_remote(q, j).wait_send()

    for it in range(ITERS):
        for d in range(1, ne):
            ps_copy(it, d).wait_send()


def hand_over(coadd_in, spec_in, morph_in, coadd_out, spec_out, morph_out, sems, row_sems):
    owned, _, pix_part = morph_out.shape
    _, held, block = morph_in.shape
    copies = [
        pltpu.make_async_copy(morph_in.at[:, row, :],
                              morph_out.at[row % owned, :, pl.ds(row // owned * block, block)],
                              row_sems.at[row])
        for row in range(held)
    ]
    copies.append(pltpu.make_async_copy(coadd_in, coadd_out, sems.at[0]))
    copies.append(pltpu.make_async_copy(spec_in, spec_out, sems.at[1]))
    for copy in copies:
        copy.start()
    for copy in copies:
        copy.wait()


def fused(ne, nb, visit_flux, visit_precision, visit_live, footprint, source_count, spectra_init,
          morphology_init):
    visits, every_blend, bands, block = visit_flux.shape
    owned, slots, pix_part = morphology_init.shape
    ny, nx = factors(ne)
    width = ne * LANES
    chunks = block // width
    per_dest = pix_part // block
    held = per_dest * owned
    hop = max(nx, ny) - 1
    line = max(nx, ny)
    f32 = jnp.float32
    vmem, smem, hbm = (pl.BlockSpec(memory_space=s) for s in (pltpu.VMEM, pltpu.SMEM, pl.ANY))
    dma = pltpu.SemaphoreType.DMA
    parts = pl.pallas_call(
        functools.partial(coadd_kernel, ne=ne, nb=nb, ny=ny, nx=nx),
        out_shape=(
            pltpu.VMEM((bands, owned, pix_part), f32),
            pltpu.VMEM((bands, owned, slots), f32),
            pltpu.VMEM((slots, held, block), f32),
        ),
        in_specs=[hbm, hbm, vmem, hbm, smem, vmem, hbm],
        out_specs=(vmem, vmem, vmem),
        scratch_shapes=[
            pltpu.VMEM((chunks, visits, bands, every_blend, width), visit_flux.dtype),
            pltpu.VMEM((chunks, visits, bands, every_blend, width), visit_precision.dtype),
            pltpu.VMEM((slots, held, block), jnp.int32),
            pltpu.VMEM((bands, held, block), f32),
            pltpu.VMEM((bands, held, block), f32),
            pltpu.VMEM((2, chunks, ne, bands, every_blend, LANES), f32),
            pltpu.VMEM((2, chunks, hop, line, bands, every_blend, LANES), f32),
            pltpu.VMEM((2, chunks, line, bands, every_blend, LANES), f32),
            pltpu.VMEM((2, chunks, hop, bands, every_blend, LANES), f32),
            pltpu.VMEM((chunks, nb, 2, bands, owned, LANES), f32),
            pltpu.VMEM((chunks, 2, bands, per_dest, owned, width), f32),
            pltpu.VMEM((slots, bands, held, LANES), f32),
            pltpu.VMEM((slots, held, LANES), f32),
            pltpu.VMEM((slots, bands + 1, held, LANES), f32),
            pltpu.VMEM((ITERS, ne, held, LANES), f32),
            dma((2, chunks)),
            dma((2, held)),
            dma((2, chunks, hop)),
            dma((2, chunks, hop)),
            dma((2, chunks, hop)),
            dma((2, chunks, hop)),
            dma((chunks, nb)),
            dma((chunks,)),
            dma((ITERS, ne - 1)),
            dma((ITERS, ne - 1)),
        ],
        compiler_params=pltpu.CompilerParams(
            collective_id=0, has_side_effects=True, vmem_limit_bytes=58 * 2**20
        ),
    )(visit_flux.transpose(0, 2, 1, 3), visit_precision.transpose(0, 2, 1, 3), visit_live,
      footprint, source_count, spectra_init.transpose(2, 0, 1), morphology_init)
    coadd, spectra, morphology = pl.pallas_call(
        hand_over,
        out_shape=(
            jax.ShapeDtypeStruct((bands, owned, pix_part), f32),
            jax.ShapeDtypeStruct((bands, owned, slots), f32),
            jax.ShapeDtypeStruct((owned, slots, pix_part), f32),
        ),
        in_specs=[vmem] * 3,
        out_specs=(hbm,) * 3,
        scratch_shapes=[dma((2,)), dma((held,))],
        compiler_params=pltpu.CompilerParams(vmem_limit_bytes=8 * 2**20),
    )(*parts)
    return coadd.transpose(1, 0, 2), spectra.transpose(1, 2, 0), morphology


def on_device(
    visit_flux, visit_precision, visit_live, footprint, source_count, spectra_init, morphology_init
):
    weights = visit_precision.astype(jnp.float32) * visit_live.astype(jnp.float32)[:, :, None, None]
    numerator = jnp.sum(weights * visit_flux.astype(jnp.float32), axis=0)
    weight_sum = jnp.sum(weights, axis=0)
    pix_part = morphology_init.shape[2]
    owned = morphology_init.shape[0]
    numerator, weight_sum = (
        lax.psum_scatter(numerator, "epoch", scatter_dimension=2, tiled=True),
        lax.psum_scatter(weight_sum, "epoch", scatter_dimension=2, tiled=True),
    )
    every_blend, band_count, piece = numerator.shape
    numerator = numerator.reshape(every_blend, band_count, 1, piece)
    weight_sum = weight_sum.reshape(every_blend, band_count, 1, piece)
    numerator, weight_sum = (
        lax.all_to_all(numerator, "blend", split_axis=0, concat_axis=2, tiled=True),
        lax.all_to_all(weight_sum, "blend", split_axis=0, concat_axis=2, tiled=True),
    )
    blocks = numerator.shape[2]
    numerator = numerator.reshape(owned, band_count, blocks, 1, piece)
    weight_sum = weight_sum.reshape(owned, band_count, blocks, 1, piece)
    numerator, weight_sum = (
        lax.all_to_all(numerator, "epoch", split_axis=2, concat_axis=3, tiled=True),
        lax.all_to_all(weight_sum, "epoch", split_axis=2, concat_axis=3, tiled=True),
    )
    numerator = numerator.reshape(owned, band_count, pix_part)
    weight_sum = weight_sum.reshape(owned, band_count, pix_part)
    coadd_flux = numerator / (1.0 + weight_sum)
    coverage = weight_sum / (1.0 + weight_sum)
    slots = footprint.shape[1]
    source_live = (jnp.arange(slots, dtype=jnp.int32)[None, :] < source_count[:, None]).astype(
        jnp.float32
    )
    footprint_mask = footprint.astype(jnp.float32) * source_live[:, :, None]
    live_count = source_count.astype(jnp.float32)
    morphology = morphology_init * footprint_mask
    spectra = spectra_init
    highest = lax.Precision.HIGHEST
    for iteration in range(ITERS):
        blend_model = jnp.einsum("bkc,bkp->bcp", spectra, morphology, precision=highest)
        residual = coverage * (coadd_flux - blend_model)
        morph_grad = jnp.einsum("bkc,bcp->bkp", spectra, residual, precision=highest)
        morph_step = 1.0 / (1.0 + live_count[:, None] * jnp.sum(spectra * spectra, axis=2))
        morphology = (
            jnp.maximum(0.0, morphology + morph_grad * morph_step[:, :, None]) * footprint_mask
        )
        blend_model = jnp.einsum("bkc,bkp->bcp", spectra, morphology, precision=highest)
        residual = coverage * (coadd_flux - blend_model)
        spectra_grad = jnp.einsum("bkp,bcp->bkc", morphology, residual, precision=highest)
        morph_norm = jnp.sum(morphology * morphology, axis=2)
        spectra_grad, morph_norm = lax.psum((spectra_grad, morph_norm), "epoch")
        spectra = jnp.maximum(
            0.0, spectra + spectra_grad / (1.0 + live_count[:, None] * morph_norm)[:, :, None]
        )
    return (coadd_flux, spectra, morphology)


def solution(mesh):
    ne, nb = mesh.shape["epoch"], mesh.shape["blend"]

    def step(visit_flux, visit_precision, visit_live, footprint, source_count, spectra_init,
             morphology_init):
        block, bands = visit_flux.shape[3], visit_flux.shape[2]
        owned, pix_part = morphology_init.shape[0], morphology_init.shape[2]
        ny, nx = factors(ne)
        fits = (
            block % (ne * LANES) == 0
            and pix_part % block == 0
            and min(ny, nx) > 1
            and morphology_init.shape[1] * (bands + 1) <= LANES
        )
        run = functools.partial(fused, ne, nb) if fits else on_device
        return run(visit_flux, visit_precision, visit_live, footprint, source_count, spectra_init,
                   morphology_init)

    in_specs = (
        P("epoch", None, None, "blend"),
        P("epoch", None, None, "blend"),
        P("epoch", None),
        P("blend", None, "epoch"),
        P("blend"),
        P("blend", None, None),
        P("blend", None, "epoch"),
    )
    out_specs = (P("blend", None, "epoch"), P("blend", None, None), P("blend", None, "epoch"))
    return jax.shard_map(
        step, mesh=mesh, in_specs=in_specs, out_specs=out_specs, check_vma=False
    )
```
